32 devices in a mesh: row: 2 (over x), col: 4 (over z), layer: 4 (over y, core).
Axes of the slice: x: 2, y: 2, z: 4, core: 2. Of those that a mesh axis runs over, the one named last changes fastest.
Arguments:
- left_factor: float32 [2048, 4096], P('row', ('layer', 'col')), may hold values from 0.01 to 1
- right_factor: float32 [4096, 4096], P(('layer', 'row'), 'col'), may hold values from 0.01 to 1
- left_occupancy: int32 [16, 32], replicated, may hold values 0 or 1
- right_occupancy: int32 [32, 32], replicated, may hold values 0 or 1
Outputs:
- flow: float32 [2048, 4096], P(('row', 'layer'), 'col')
The draws below stay inside these ranges and needn't reach their ends.
All inputs are finite; a program needn't handle non-finite values.
Results may differ from the reference program's by a relative error of at most 0.000082.
Values sent between devices are 32-bit elements; how exact they have to be, the bound alone decides.
No kernel may reach another device: no remote copies, remote signals or barrier semaphores. Data moves between devices by JAX's collectives and lax.ppermute only.
A program may use at most 64 MiB of HBM per device.

```python
import math
import jax
import jax.numpy as jnp
from jax import lax

BLOCK = 128
K = 4096
ROWS = 2048
COLS = 4096


def place_ends(array, stream_key, least, top_value):
    index_at = [jax.random.randint(jax.random.fold_in(stream_key, axis), (), 0, length) for axis, length in enumerate(array.shape)]
    main_axis = array.shape.index(max(array.shape))
    next_to = index_at[:main_axis] + [(index_at[main_axis] + 1) % array.shape[main_axis]] + index_at[main_axis + 1:]
    return array.at[tuple(index_at)].set(least).at[tuple(next_to)].set(top_value)


def levels(stream_key, extent, cuts, smallest, high):
    gain, own = 1.0, jax.random.fold_in(stream_key, 6)
    for dim, shards_of in cuts:
        heights = jnp.exp(jax.random.uniform(jax.random.fold_in(own, dim), (shards_of,), jnp.float32, smallest / len(cuts), high / len(cuts)))
        gain = gain * jnp.repeat(heights, extent[dim] // shards_of).reshape([-1 if axis == dim else 1 for axis in range(len(extent))])
    return gain


def setup_inputs(seed: int = 0) -> dict:
    streams_of = jax.random.split(jax.random.key(seed), 5)
    return {
        "left_factor": jnp.clip(jnp.exp(math.log(1.0) - 4.6051702 * jax.random.uniform(streams_of[0], (ROWS, K), jnp.float32) ** levels(streams_of[0], (ROWS, K), ((0, 2), (1, 16)), -0.2, 0.2)), 0.01, 1.0),
        "right_factor": jnp.clip(jnp.exp(math.log(1.0) - 4.6051702 * jax.random.uniform(streams_of[1], (K, COLS), jnp.float32) ** levels(streams_of[1], (K, COLS), ((0, 8), (1, 4)), -0.2, 0.2)), 0.01, 1.0),
        "left_occupancy": place_ends((jax.random.randint(streams_of[2], (ROWS // BLOCK, K // BLOCK), 0, 4) < 3).astype(jnp.int32), jax.random.fold_in(streams_of[2], 1), 0, 1),
        "right_occupancy": place_ends((jax.random.randint(streams_of[3], (K // BLOCK, COLS // BLOCK), 0, 4) < 3).astype(jnp.int32), jax.random.fold_in(streams_of[3], 1), 0, 1),
    }


EPSILON = 1e-6


def widen(flags):
    return jnp.repeat(jnp.repeat(flags.astype(jnp.float32), BLOCK, 0), BLOCK, 1)


def reference(left_factor, right_factor, left_occupancy, right_occupancy):
    left_sparse = left_factor * widen(left_occupancy)
    right_sparse = right_factor * widen(right_occupancy)
    expanded = jnp.dot(left_sparse, right_sparse, precision=lax.Precision.HIGHEST, preferred_element_type=jnp.float32)
    squared = expanded * expanded
    totals = jnp.sum(squared, axis=0)
    return ROWS * squared / (totals + EPSILON)
```

```python
import functools

import jax
import jax.numpy as jnp
from jax import lax
from jax.experimental import pallas as pl
from jax.experimental.pallas import tpu as pltpu
from jax.sharding import PartitionSpec as P

BLOCK = 128
TILE = 256
EPSILON = 1e-06
CUTS = (5, 6, 7, 8)


def split(x):
    high = x.astype(jnp.bfloat16)
    low = (x - high.astype(jnp.float32)).astype(jnp.bfloat16)
    return high, low


def spans(start, stop):
    edges = [start, *(e for e in range(0, stop, BLOCK) if start < e), stop]
    return list(zip(edges[:-1], edges[1:]))


def right_kernel(place, flags, x_ref, *refs, depth):
    high_ref, low_ref = refs[-2:]
    rows, cols = x_ref.shape
    first = place[0] * depth + place[2] * rows
    column = place[1] * (pl.num_programs(0) * cols) + pl.program_id(0) * cols
    for r, r1 in spans(0, rows):
        for c in range(0, cols, BLOCK):
            flag = flags[(first + r) // BLOCK, (column + c) // BLOCK].astype(jnp.float32)
            high, low = split(x_ref[r:r1, c : c + BLOCK] * flag)
            high_ref[r:r1, c : c + BLOCK] = high
            low_ref[r:r1, c : c + BLOCK] = low


def prepare_right(piece, place, flags, depth, before):
    rows, cols = piece.shape
    spec = pl.BlockSpec((rows, TILE), lambda j, place, flags: (place[2], j))
    out = jax.ShapeDtypeStruct((depth, cols), jnp.bfloat16)
    return pl.pallas_call(
        functools.partial(right_kernel, depth=depth),
        grid_spec=pltpu.PrefetchScalarGridSpec(
            num_scalar_prefetch=2,
            grid=(cols // TILE,),
            in_specs=[pl.BlockSpec((rows, TILE), lambda j, place, flags: (0, j))]
            + [pl.BlockSpec(memory_space=pl.ANY)] * len(before),
            out_specs=[spec, spec],
        ),
        out_shape=[out, out],
        input_output_aliases={3 + i: i for i in range(len(before))},
        name="prepare_right",
    )(place, flags, piece, *before)


def product_kernel(place, flags, *refs, start, n_col, own_rows):
    row, col, layer = place[0], place[1], place[2]
    n_in = 2 * n_col - 1
    own, lefts, rights = refs[0], refs[1:n_col], refs[n_col:n_in]
    bh_ref, bl_ref, keep_ref, send_ref, ah_ref, al_ref = refs[n_in:]
    n_layer, size, width = own.shape
    depth = n_col * width

    @pl.when(pl.program_id(0) == 0)
    def _():
        for d in range(n_col):
            source = lax.rem(col - d + n_col, n_col)
            for l in range(n_layer):
                base = (row * n_layer + l) * own_rows
                for r, r1 in spans(start, start + size):
                    for k in range(0, width, BLOCK):
                        k1 = min(k + BLOCK, width)
                        at = (l, slice(r - start, r1 - start), slice(k, k1))
                        x = own[at] if d == 0 else lefts[d - 1][at] + rights[n_col - d - 1][at]
                        flag = flags[(base + r) // BLOCK, (layer * depth + source * width + k) // BLOCK]
                        high, low = split(x * flag.astype(jnp.float32))
                        to = (d, slice(l * size + r - start, l * size + r1 - start), slice(k, k1))
                        ah_ref[to] = high
                        al_ref[to] = low

    total = None
    for d in range(n_col):
        source = lax.rem(col - d + n_col, n_col)
        rows = pl.ds(pl.multiple_of(source * width, width), width)
        bh, bl = bh_ref[rows, :], bl_ref[rows, :]
        ah, al = ah_ref[d], al_ref[d]
        part = (
            jnp.dot(ah, bh, preferred_element_type=jnp.float32)
            + jnp.dot(ah, bl, preferred_element_type=jnp.float32)
            + jnp.dot(al, bh, preferred_element_type=jnp.float32)
        )
        total = part if total is None else total + part
    odd = lax.rem(layer, 2) == 1
    for h in range(n_layer // 2):
        zero = total[2 * h * size : (2 * h + 1) * size]
        one = total[(2 * h + 1) * size : (2 * h + 2) * size]
        keep_ref[h] = jnp.where(odd, one, zero)
        send_ref[h] = jnp.where(odd, zero, one)


def product(own, lefts, rights, b_high, b_low, place, flags, start, own_rows):
    n_layer, size, width = own.shape
    n_col = len(lefts) + 1
    depth, cols = b_high.shape
    a_spec = pl.BlockSpec((n_layer, size, width), lambda j, place, flags: (0, 0, 0))
    b_spec = pl.BlockSpec((depth, TILE), lambda j, place, flags: (0, j))
    o_spec = pl.BlockSpec((n_layer // 2, size, TILE), lambda j, place, flags: (0, 0, j))
    out = jax.ShapeDtypeStruct((n_layer // 2, size, cols), jnp.float32)
    return pl.pallas_call(
        functools.partial(product_kernel, start=start, n_col=n_col, own_rows=own_rows),
        grid_spec=pltpu.PrefetchScalarGridSpec(
            num_scalar_prefetch=2,
            grid=(cols // TILE,),
            in_specs=[a_spec] * (2 * n_col - 1) + [b_spec, b_spec],
            out_specs=[o_spec, o_spec],
            scratch_shapes=[pltpu.VMEM((n_col, n_layer * size, width), jnp.bfloat16)] * 2,
        ),
        out_shape=[out, out],
        cost_estimate=pl.CostEstimate(
            flops=6 * n_layer * size * depth * cols, bytes_accessed=4 * depth * cols, transcendentals=0
        ),
        name="product",
    )(place, flags, own, *lefts, *rights, b_high, b_low)


def on_device(left, right, left_flags, right_flags, *, sizes):
    n_row, n_col, n_layer = sizes
    row, col, layer = (lax.axis_index(a) for a in ("row", "col", "layer"))
    band, width = left.shape
    depth = n_col * width
    own_rows = band // n_layer

    rights = [
        (lax.ppermute(right, "row", [(i, (i + k) % n_row) for i in range(n_row)]), lax.rem(row - k + n_row, n_row))
        for k in range(1, n_row)
    ]
    cuts = [0] + [own_rows * c // CUTS[-1] for c in CUTS]
    bands = left.reshape(n_layer, own_rows, width)
    moved = []
    for s0, s1 in zip(cuts[:-1], cuts[1:]):
        own = bands[:, s0:s1]
        ups, downs, up, down = [], [], own, own
        for d in range(1, n_col):
            up = lax.ppermute(up, "col", [(i, i + 1) for i in range(d - 1, n_col - 1)])
            down = lax.ppermute(down, "col", [(i + 1, i) for i in range(n_col - d)])
            ups.append(up)
            downs.append(down)
        moved.append((own, ups, downs))

    before = ()
    for piece, source in [(right, row), *rights]:
        place = jnp.stack([layer, col, source])
        before = prepare_right(piece, place, right_flags, depth, before)
    place = jnp.stack([row, col, layer])
    owned = []
    for s0, (own, ups, downs) in zip(cuts[:-1], moved):
        keep, send = product(own, ups, downs, *before, place, left_flags, s0, own_rows)
        bit = 1
        while True:
            got = lax.ppermute(send, "layer", [(i, i ^ bit) for i in range(n_layer)])
            bit *= 2
            if bit == n_layer:
                owned.append((keep + got)[0])
                break
            total = (keep + got).reshape(-1, 2, *keep.shape[1:])
            mine = lax.rem(layer // bit, 2)
            keep = lax.dynamic_index_in_dim(total, mine, 1, False)
            send = lax.dynamic_index_in_dim(total, 1 - mine, 1, False)
    expanded = jnp.concatenate(owned, 0)
    squared = expanded * expanded
    totals = jnp.sum(squared, axis=0, keepdims=True)
    for axis, n in (("layer", n_layer), ("row", n_row)):
        bit = 1
        while bit < n:
            totals = totals + lax.ppermute(totals, axis, [(i, i ^ bit) for i in range(n)])
            bit *= 2
    return (band * n_row) * squared / (totals + EPSILON)


def solution(mesh):
    sizes = tuple(mesh.shape[a] for a in ("row", "col", "layer"))
    return jax.shard_map(
        functools.partial(on_device, sizes=sizes),
        mesh=mesh,
        in_specs=(P("row", ("layer", "col")), P(("layer", "row"), "col"), P(), P()),
        out_specs=P(("row", "layer"), "col"),
        check_vma=False,
    )
```
